32 devices in a mesh: grp: 4 (over y, x), mem: 8 (over z, core).
Axes of the slice: x: 2, y: 2, z: 4, core: 2. Of those that a mesh axis runs over, the one named last changes fastest.
Arguments:
- weight: bfloat16 [2, 16384, 16384], P(None, None, ('grp', 'mem')), may hold values from -0.046875 to 0.046875
- activation: bfloat16 [2, 16384, 512], P(None, ('grp', 'mem')), may hold values from -6 to 6
- points: int32 [4], replicated, may hold values from 0 to 3, each once
Outputs:
- share: float32 [4, 16384, 512], P('grp', 'mem')
The draws below stay inside these ranges and needn't reach their ends.
Inputs may be any that keep to these rules, and one draw needn't show every extreme that they name: A permutation of 0 to 3; group g evaluates at points[g] + 1.
All inputs are finite; a program needn't handle non-finite values.
Results may differ from the reference program's by a relative error of at most 0.0042.
Values may be sent and summed in bfloat16 or wider, within the bound.
A program may use at most 320 MiB of HBM per device.

```python
import jax
import jax.numpy as jnp

D = 16384
C = 512
SPLITS = 2
BLOCKS = 2
FB = 16384
N_GRP = 4


def steps_of(own_key, extent, cuts, low, high):
    level = 1.0
    for dim, blocks in cuts:
        steps = jax.random.uniform(jax.random.fold_in(jax.random.fold_in(own_key, 6), dim), (blocks,), jnp.float32, low / len(cuts), high / len(cuts))
        level = level * jnp.repeat(jnp.exp(steps), extent[dim] // blocks).reshape((-1,) + (1,) * (len(extent) - 1 - dim))
    return level


def scatter_about(stream_key, dims, width, bound, cuts=(), held_as=jnp.bfloat16):
    entries = width * jax.random.normal(stream_key, dims, jnp.float32)
    if cuts:
        entries = entries * steps_of(stream_key, dims, cuts, -0.22, 0.18)
    return jnp.clip(entries, -bound, bound).astype(held_as)


def setup_inputs(seed: int = 0) -> dict:
    keys = jax.random.split(jax.random.key(seed), 4)
    weight = scatter_about(keys[0], (BLOCKS, FB, D), D ** -0.5, 0.046875, ((2, 32),))
    activation = scatter_about(keys[1], (SPLITS, D, C), 1.0, 6.0, ((1, 32),))
    points = jax.random.permutation(keys[2], N_GRP).astype(jnp.int32)
    return {"weight": weight, "activation": activation, "points": points}


def reference(weight, activation, points):
    anchors = (points + 1).astype(jnp.float32) / N_GRP
    weight_powers = jnp.arange(BLOCKS, dtype=jnp.float32)
    input_powers = jnp.arange(SPLITS, dtype=jnp.float32) * BLOCKS
    shares = []
    for group in range(N_GRP):
        factors = anchors[group] ** weight_powers
        total = factors[0] * weight[0].astype(jnp.float32)
        for block in range(1, BLOCKS):
            total = total + factors[block] * weight[block].astype(jnp.float32)
        coded_weight = total.astype(jnp.bfloat16)
        lifts = anchors[group] ** input_powers
        mixed = lifts[0] * activation[0].astype(jnp.float32)
        for split in range(1, SPLITS):
            mixed = mixed + lifts[split] * activation[split].astype(jnp.float32)
        coded_input = mixed.astype(jnp.bfloat16)
        shares.append(jnp.dot(coded_weight, coded_input, preferred_element_type=jnp.float32))
    return jnp.stack(shares)
```

```python
import jax
import jax.numpy as jnp
from jax import lax
from jax.experimental import pallas as pl
from jax.experimental.pallas import tpu as pltpu
from jax.sharding import PartitionSpec as P

PAIRS = 4
F32, BF16 = jnp.float32, jnp.bfloat16
MESH = pl.DeviceIdType.MESH


def loop(n, body):
    def step(i, carry):
        body(i)
        return carry

    lax.fori_loop(0, n, step, 0)


def make_kernel(groups, members, blocks, splits, rows, depth, cols, ra, rb):
    bits = groups.bit_length() - 1
    ring = members // 2
    half = groups // 2
    off = [groups - (groups >> s) for s in range(bits + 1)]

    def kernel(points, weight, act, out, wxa, wxb, xp, xs, wt, cw, asend, az, ag, bsend, bg, bz,
               x_s, x_r, w_s, wa_r, wb_r, ld, send, az_r, ag_r, bg_r, bz_r):
        me_g = lax.axis_index("grp")
        me_m = lax.axis_index("mem")
        z, core = me_m // 2, me_m % 2
        twin = (me_g, z * 2 + 1 - core)

        def along(sgn):
            return (me_g, ((z + sgn + ring) % ring) * 2 + core)

        def blend(o, v0, v1):
            return v0 + o * (v1 - v0)

        def bit_of(w):
            return (me_g // w) % 2

        def across(o, s):
            w0, w1 = 1 << (bits - 1 - s), 1 << s
            p0 = me_g + w0 - 2 * w0 * bit_of(w0)
            p1 = me_g + w1 - 2 * w1 * bit_of(w1)
            return (blend(o, p0, p1), me_m)

        def group_at(o, s, h, j):
            w0, w1 = 1 << (bits - 1 - s), 1 << s
            b0, b1 = bit_of(w0), bit_of(w1)
            b0, b1 = b0 + h - 2 * b0 * h, b1 + h - 2 * b1 * h
            g0 = (me_g // (2 * w0)) * (2 * w0) + b0 * w0 + j
            g1 = me_g % w1 + b1 * w1 + j * (2 * w1)
            return blend(o, g0, g1)

        def slot_at(o, s, h, j):
            w0, w1 = 1 << (bits - 1 - s), 1 << s
            b0, b1 = bit_of(w0), bit_of(w1)
            b0, b1 = b0 + h - 2 * b0 * h, b1 + h - 2 * b1 * h
            return blend(o, b0 * w0 + j, b1 + 2 * j)

        def remote(src, dst, ssem, rsem, dev):
            return pltpu.make_async_remote_copy(
                src_ref=src, dst_ref=dst, send_sem=ssem, recv_sem=rsem, device_id=dev, device_id_type=MESH)

        def arrived(ref, sem):
            pltpu.make_async_copy(ref, ref, sem).wait()

        def anchor(g):
            return (points[g] + 1).astype(F32) / groups

        def power(a, n):
            r = a
            for _ in range(n - 1):
                r = r * a
            return r

        barrier = pltpu.get_barrier_semaphore()
        peers = [twin, along(1), along(-1)] + [across(0, s) for s in range(bits)]
        for dev in peers:
            pl.semaphore_signal(barrier, inc=1, device_id=dev, device_id_type=MESH)
        pl.semaphore_wait(barrier, len(peers))

        def a_sign(c):
            return 1 - 2 * c

        def b_sign(c):
            return 1 - 2 * ((c % 2 + c // 2) % 2)

        def dest(sgn, t):
            return (z - sgn * (1 + t) + 2 * ring) % ring

        def base(is_a, c, zd, core_):
            lead = c * ra if is_a else 2 * ra + c * rb
            return pl.multiple_of((zd * 2 + core_) * rows + lead, 16)

        x_copy = remote(act, xp, x_s, x_r, twin)
        x_copy.start()

        def push_a(t):
            def body(c):
                zd = dest(a_sign(c), t)
                remote(weight.at[:, pl.ds(base(True, c, zd, 1 - core), ra), :], wxa.at[c, t],
                       w_s.at[0], wa_r.at[c, t], twin).start()
            loop(2, body)

        def push_b(c):
            def body(t):
                zd = dest(b_sign(c), t)
                remote(weight.at[:, pl.ds(base(False, c, zd, 1 - core), rb), :], wxb.at[c, t],
                       w_s.at[1], wb_r.at[c], twin).start()
            loop(ring, body)

        push_a(0)
        push_b(0)
        push_b(1)
        if ring > 2:
            push_a(1)
        loop(2 * PAIRS - 2, lambda c: push_b(c + 2))
        for t in range(2, ring):
            push_a(t)

        x_copy.wait_recv()
        step = min(32, depth)

        def code_input(g):
            lift = power(anchor(g), blocks)
            for h, src in enumerate((act, xp)):
                def body(r):
                    at = pl.ds(pl.multiple_of(r * step, step), step)
                    total = src[0, at, :].astype(F32)
                    for k in range(1, splits):
                        total = total + power(lift, k) * src[k, at, :].astype(F32)
                    xs[g, pl.ds(pl.multiple_of(h * depth + r * step, step), step), :] = total.astype(BF16)
                loop(depth // step, body)
        loop(groups, code_input)

        def tile_copies(is_a, c, t, sgn, slot):
            n = ra if is_a else rb
            wx = wxa if is_a else wxb
            own = pltpu.make_async_copy(
                weight.at[:, pl.ds(base(is_a, c, dest(sgn, t), core), n), :],
                wt.at[slot, 0, :, pl.ds(0, n), :], ld.at[slot, 0])
            other = pltpu.make_async_copy(wx.at[c, t], wt.at[slot, 1, :, pl.ds(0, n), :], ld.at[slot, 1])
            return own, other

        def product(slot, n, g):
            a = anchor(g)
            factors = [power(a, j) for j in range(1, blocks)]

            def body(r):
                at = pl.ds(pl.multiple_of(r * 16, 16), 16)
                for h in range(2):
                    total = wt[slot, h, 0, at, :].astype(F32)
                    for j in range(1, blocks):
                        total = total + factors[j - 1] * wt[slot, h, j, at, :].astype(F32)
                    cw[at, h * depth:(h + 1) * depth] = total.astype(BF16)
            loop(n // 16, body)
            return jnp.dot(cw[0:n, :], xs[g], preferred_element_type=F32)

        def a_hop(t):
            def body(c, slot):
                def per_group(g):
                    acc = product(slot, ra, g)
                    if t == 0:
                        src = asend.at[c, g]
                        asend[c, g] = acc.astype(BF16)
                    else:
                        src = az.at[c, t - 1, g]
                        arrived(src, az_r.at[c, t - 1, g])
                        az[c, t - 1, g] = (acc + az[c, t - 1, g].astype(F32)).astype(BF16)
                    remote(src, az.at[c, t, g], send.at[0 if t == 0 else 1], az_r.at[c, t, g],
                           along(a_sign(c))).start()
                loop(groups, per_group)
            return body

        def a_turn(c, slot):
            def per_group(i):
                h, j = 1 - i // half, i % half
                g = group_at(c, 0, h, j)
                acc = product(slot, ra, g)
                arrived(az.at[c, ring - 2, g], az_r.at[c, ring - 2, g])
                az[c, ring - 2, g] = (acc + az[c, ring - 2, g].astype(F32)).astype(BF16)

                @pl.when(i < half)
                def _():
                    remote(az.at[c, ring - 2, g], ag.at[c, j], send.at[2], ag_r.at[c, 0], across(c, 0)).start()
            loop(groups, per_group)

        def a_stage(s):
            def body(c):
                n = half >> (s - 1)
                arrived(ag.at[c, pl.ds(off[s - 1], n)], ag_r.at[c, s - 1])

                def held(j):
                    if s == 1:
                        return az[c, ring - 2, group_at(c, 0, 0, j)]
                    return ag[c, off[s - 2] + slot_at(c, s - 1, 0, j)]

                def summed(j):
                    return ag[c, off[s - 1] + j].astype(F32) + held(j).astype(F32)

                if s == bits:
                    out[0, pl.ds(pl.multiple_of(c * ra, 16), ra), :] = summed(0)
                    return

                def per_slot(i):
                    h, jj = 1 - i // (n // 2), i % (n // 2)
                    j = slot_at(c, s, h, jj)
                    ag[c, off[s - 1] + j] = summed(j).astype(BF16)

                    @pl.when(i < n // 2)
                    def _():
                        remote(ag.at[c, off[s - 1] + j], ag.at[c, off[s] + jj], send.at[3],
                               ag_r.at[c, s], across(c, s)).start()
                loop(n, per_slot)
            return body

        def b_first(c, t, slot):
            o = c % 2

            def per_slot(j):
                acc = product(slot, rb, group_at(o, 0, 1, j))
                bsend[c, t, j] = acc.astype(BF16)
                remote(bsend.at[c, t, j], bg.at[c, t, j], send.at[4], bg_r.at[c, t, 0], across(o, 0)).start()
            loop(half, per_slot)

        def b_merge(c, t, s, add):
            o = c % 2
            n = half >> (s - 1)
            arrived(bg.at[c, t, pl.ds(off[s - 1], n)], bg_r.at[c, t, s - 1])

            def per_slot(i):
                h, jj = 1 - i // (n // 2), i % (n // 2)
                j = slot_at(o, s, h, jj)
                bg[c, t, off[s - 1] + j] = (add(j) + bg[c, t, off[s - 1] + j].astype(F32)).astype(BF16)

                @pl.when(i < n // 2)
                def _():
                    remote(bg.at[c, t, off[s - 1] + j], bg.at[c, t, off[s] + jj], send.at[5],
                           bg_r.at[c, t, s], across(o, s)).start()
            loop(n, per_slot)

        def b_second(c, t, slot):
            b_merge(c, t, 1, lambda j: product(slot, rb, group_at(c % 2, 0, 0, j)))

        def b_middle(p, s):
            def body(i):
                c, t = 2 * p + i % 2, i // 2
                b_merge(c, t, s, lambda j: bg[c, t, off[s - 2] + slot_at(c % 2, s - 1, 0, j)].astype(F32))
            loop(2 * ring, body)

        def b_ring(p, t):
            def body(i):
                c = 2 * p + i
                last = off[bits - 1]
                arrived(bg.at[c, t, pl.ds(last, 1)], bg_r.at[c, t, bits - 1])
                kept = off[bits - 2] + slot_at(c % 2, bits - 1, 0, 0)
                val = bg[c, t, last].astype(F32) + bg[c, t, kept].astype(F32)
                if t > 0:
                    arrived(bz.at[c, t - 1], bz_r.at[c, t - 1])
                    val = val + bz[c, t - 1].astype(F32)
                if t == ring - 1:
                    out[0, pl.ds(pl.multiple_of(2 * ra + c * rb, 16), rb), :] = val
                    return
                if t == 0:
                    src = bg.at[c, t, last]
                    bg[c, t, last] = val.astype(BF16)
                else:
                    src = bz.at[c, t - 1]
                    bz[c, t - 1] = val.astype(BF16)
                remote(src, bz.at[c, t], send.at[6], bz_r.at[c, t], along(b_sign(c))).start()
            loop(2, body)

        def a_site(t, body):
            return ("tiles", True, True, 2, lambda i: (i, t), lambda c, t_, slot: body(c, slot))

        def b_site(p, first, body):
            return ("tiles", False, first, 2 * ring, lambda i: (2 * p + i % 2, i // 2), body)

        def plain(fn):
            return ("plain", fn)

        a_queue = [a_site(t, a_hop(t)) for t in range(1, ring - 1)] + [a_site(ring - 1, a_turn)]
        a_queue += [plain(lambda s=s: loop(2, a_stage(s))) for s in range(1, bits + 1)]
        queues, order = [], [a_site(0, a_hop(0))]

        def drain(with_a):
            for q in queues:
                if q:
                    order.append(q.pop(0))
            if with_a and a_queue:
                order.append(a_queue.pop(0))

        for p in range(PAIRS):
            order.append(b_site(p, True, b_first))
            drain(p == 1 or p > 2)
            order.append(b_site(p, False, b_second))
            drain(p > 0)
            queues.append([plain(lambda p=p, s=s: b_middle(p, s)) for s in range(2, bits)]
                          + [plain(lambda p=p, t=t: b_ring(p, t)) for t in range(ring)])
        while a_queue or any(queues):
            drain(True)

        def begin(site, i, slot):
            _, is_a, first, _, index, _ = site
            c, t = index(i)
            sgn = a_sign(c) if is_a else b_sign(c)
            own, other = tile_copies(is_a, c, t, sgn, slot)
            own.start()
            if is_a:
                arrived(wxa.at[c, t], wa_r.at[c, t])
            elif first:
                @pl.when(t == 0)
                def _():
                    arrived(wxb.at[c], wb_r.at[c])
            other.start()

        tiles = [s for s in order if s[0] == "tiles"]
        begin(tiles[0], 0, 0)
        at = 0
        for site in order:
            if site[0] == "plain":
                site[1]()
                continue
            at += 1
            follow = tiles[at] if at < len(tiles) else None
            _, is_a, first, count, index, body = site

            def run(i, site=site, follow=follow, is_a=is_a, count=count, index=index, body=body):
                slot = i % 2

                @pl.when(i + 1 < count)
                def _():
                    begin(site, i + 1, 1 - slot)

                if follow is not None:
                    @pl.when(i + 1 == count)
                    def _():
                        begin(follow, 0, 1 - slot)
                c, t = index(i)
                for cp in tile_copies(is_a, c, t, a_sign(c) if is_a else b_sign(c), slot):
                    cp.wait()
                body(c, t, slot)
            loop(count, run)

        x_copy.wait_send()
        arrived(wxa, w_s.at[0])
        arrived(wxb, w_s.at[1])
        arrived(asend, send.at[0])
        arrived(az.at[:, pl.ds(0, ring - 2)], send.at[1])
        arrived(ag.at[:, pl.ds(0, half)], send.at[2])
        arrived(ag.at[:, pl.ds(0, half - 1)], send.at[3])
        arrived(bsend, send.at[4])
        arrived(bg.at[:, :, pl.ds(0, half - 1)], send.at[5])
        arrived(bz, send.at[6])

    dma = pltpu.SemaphoreType.DMA
    nb = 2 * PAIRS
    shapes = [
        pltpu.VMEM((splits, depth, cols), BF16),
        pltpu.VMEM((groups, 2 * depth, cols), BF16),
        pltpu.VMEM((2, 2, blocks, max(ra, rb), depth), BF16),
        pltpu.VMEM((max(ra, rb), 2 * depth), BF16),
        pltpu.VMEM((2, groups, ra, cols), BF16),
        pltpu.VMEM((2, ring - 1, groups, ra, cols), BF16),
        pltpu.VMEM((2, groups - 1, ra, cols), BF16),
        pltpu.VMEM((nb, ring, half, rb, cols), BF16),
        pltpu.VMEM((nb, ring, groups - 1, rb, cols), BF16),
        pltpu.VMEM((nb, ring - 1, rb, cols), BF16),
        dma, dma, dma((2,)), dma((2, ring)), dma((nb,)), dma((2, 2)), dma((7,)),
        dma((2, ring - 1, groups)), dma((2, bits)), dma((nb, ring, bits)), dma((nb, ring - 1)),
    ]
    spaces = (pltpu.VMEM, pl.ANY, pl.ANY)
    return pl.pallas_call(
        kernel,
        name="coded_share",
        out_shape=(
            jax.ShapeDtypeStruct((1, rows, cols), F32),
            jax.ShapeDtypeStruct((2, ring, blocks, ra, depth), BF16),
            jax.ShapeDtypeStruct((nb, ring, blocks, rb, depth), BF16),
        ),
        in_specs=[
            pl.BlockSpec(memory_space=pltpu.SMEM),
            pl.BlockSpec(memory_space=pl.ANY),
            pl.BlockSpec(memory_space=pltpu.VMEM),
        ],
        out_specs=tuple(pl.BlockSpec(memory_space=m) for m in spaces),
        scratch_shapes=shapes,
        compiler_params=pltpu.CompilerParams(
            collective_id=0, has_side_effects=True, vmem_limit_bytes=67043328),
    )


def solution(mesh):
    groups, members = mesh.shape["grp"], mesh.shape["mem"]

    def per_device(weight, activation, points):
        blocks, height, depth = weight.shape
        splits, _, cols = activation.shape
        rows = height // members
        rb = (rows * 13 // 16) // (2 * PAIRS) // 16 * 16
        ra = (rows - 2 * PAIRS * rb) // 2
        call = make_kernel(groups, members, blocks, splits, rows, depth, cols, ra, rb)
        return call(points, weight, activation)[0]

    placed = (P(None, None, ("grp", "mem")), P(None, ("grp", "mem"), None), P())
    return jax.shard_map(
        per_device, mesh=mesh, in_specs=placed, out_specs=P("grp", "mem", None), check_vma=False)
```

```python
import jax
import jax.numpy as jnp
from jax import lax
from jax.experimental import pallas as pl
from jax.experimental.pallas import tpu as pltpu
from jax.sharding import PartitionSpec as P

PAIRS = 4
F32, BF16 = jnp.float32, jnp.bfloat16
MESH = pl.DeviceIdType.MESH


def loop(n, body):
    def step(i, carry):
        body(i)
        return carry

    lax.fori_loop(0, n, step, 0)


def make_kernel(groups, members, blocks, splits, rows, depth, cols, ra, rb):
    bits = groups.bit_length() - 1
    ring = members // 2
    half = groups // 2
    off = [groups - (groups >> s) for s in range(bits + 1)]

    def kernel(points, weight, act, out, wxa, wxb, xp, xs, wt, cw, asend, az, ag, bsend, bg, bz,
               x_s, x_r, w_s, wa_r, wb_r, ld, send, az_r, ag_r, bg_r, bz_r):
        me_g = lax.axis_index("grp")
        me_m = lax.axis_index("mem")
        z, core = me_m // 2, me_m % 2
        twin = (me_g, z * 2 + 1 - core)

        def along(sgn):
            return (me_g, ((z + sgn + ring) % ring) * 2 + core)

        def blend(o, v0, v1):
            return v0 + o * (v1 - v0)

        def bit_of(w):
            return (me_g // w) % 2

        def across(o, s):
            w0, w1 = 1 << (bits - 1 - s), 1 << s
            p0 = me_g + w0 - 2 * w0 * bit_of(w0)
            p1 = me_g + w1 - 2 * w1 * bit_of(w1)
            return (blend(o, p0, p1), me_m)

        def group_at(o, s, h, j):
            w0, w1 = 1 << (bits - 1 - s), 1 << s
            b0, b1 = bit_of(w0), bit_of(w1)
            b0, b1 = b0 + h - 2 * b0 * h, b1 + h - 2 * b1 * h
            g0 = (me_g // (2 * w0)) * (2 * w0) + b0 * w0 + j
            g1 = me_g % w1 + b1 * w1 + j * (2 * w1)
            return blend(o, g0, g1)

        def slot_at(o, s, h, j):
            w0, w1 = 1 << (bits - 1 - s), 1 << s
            b0, b1 = bit_of(w0), bit_of(w1)
            b0, b1 = b0 + h - 2 * b0 * h, b1 + h - 2 * b1 * h
            return blend(o, b0 * w0 + j, b1 + 2 * j)

        def remote(src, dst, ssem, rsem, dev):
            return pltpu.make_async_remote_copy(
                src_ref=src, dst_ref=dst, send_sem=ssem, recv_sem=rsem, device_id=dev, device_id_type=MESH)

        def arrived(ref, sem):
            pltpu.make_async_copy(ref, ref, sem).wait()

        def anchor(g):
            return (points[g] + 1).astype(F32) / groups

        def power(a, n):
            r = a
            for _ in range(n - 1):
                r = r * a
            return r

        barrier = pltpu.get_barrier_semaphore()
        peers = [twin, along(1), along(-1)] + [across(0, s) for s in range(bits)]
        for dev in peers:
            pl.semaphore_signal(barrier, inc=1, device_id=dev, device_id_type=MESH)
        pl.semaphore_wait(barrier, len(peers))

        def a_sign(c):
            return 1 - 2 * c

        def b_sign(c):
            return 1 - 2 * ((c % 2 + c // 2) % 2)

        def dest(sgn, t):
            return (z - sgn * (1 + t) + 2 * ring) % ring

        def base(is_a, c, zd, core_):
            lead = c * ra if is_a else 2 * ra + c * rb
            return pl.multiple_of((zd * 2 + core_) * rows + lead, 16)

        x_copy = remote(act, xp, x_s, x_r, twin)
        x_copy.start()

        def push_a(t):
            def body(c):
                zd = dest(a_sign(c), t)
                remote(weight.at[:, pl.ds(base(True, c, zd, 1 - core), ra), :], wxa.at[c, t],
                       w_s.at[0], wa_r.at[c, t], twin).start()
            loop(2, body)

        def push_b(c):
            def body(t):
                zd = dest(b_sign(c), t)
                remote(weight.at[:, pl.ds(base(False, c, zd, 1 - core), rb), :], wxb.at[c, t],
                       w_s.at[1], wb_r.at[c], twin).start()
            loop(ring, body)

        push_b(0)
        push_b(1)
        push_a(0)
        if ring > 2:
            push_a(1)
        loop(2 * PAIRS - 2, lambda c: push_b(c + 2))
        for t in range(2, ring):
            push_a(t)

        step = min(16, depth)
        lifts = [power(anchor(g), blocks) for g in range(groups)]

        def code_input(h, src):
            def body(r):
                at = pl.ds(pl.multiple_of(r * step, step), step)
                to = pl.ds(pl.multiple_of(h * depth + r * step, step), step)
                parts = [src[k, at, :].astype(F32) for k in range(splits)]
                for g in range(groups):
                    total = parts[0]
                    for k in range(1, splits):
                        total = total + power(lifts[g], k) * parts[k]
                    xs[g, to, :] = total.astype(BF16)
            loop(depth // step, body)

        code_input(0, act)
        x_copy.wait_recv()
        code_input(1, xp)

        def tile_copies(is_a, c, t, sgn, slot):
            n = ra if is_a else rb
            wx = wxa if is_a else wxb
            own = pltpu.make_async_copy(
                weight.at[:, pl.ds(base(is_a, c, dest(sgn, t), core), n), :],
                wt.at[slot, 0, :, pl.ds(0, n), :], ld.at[slot, 0])
            other = pltpu.make_async_copy(wx.at[c, t], wt.at[slot, 1, :, pl.ds(0, n), :], ld.at[slot, 1])
            return own, other

        def product(slot, n, g):
            a = anchor(g)
            factors = [power(a, j) for j in range(1, blocks)]

            def body(r):
                at = pl.ds(r * 16, 16)
                for h in range(2):
                    total = wt[slot, h, 0, at, :].astype(F32)
                    for j in range(1, blocks):
                        total = total + factors[j - 1] * wt[slot, h, j, at, :].astype(F32)
                    cw[at, h * depth:(h + 1) * depth] = total.astype(BF16)
            for r in range(n // 16):
                body(r)
            return jnp.dot(cw[0:n, :], xs[g], preferred_element_type=F32)

        def a_hop(t):
            def body(c, slot):
                def per_group(g):
                    acc = product(slot, ra, g)
                    if t == 0:
                        src = asend.at[c, g]
                        asend[c, g] = acc.astype(BF16)
                    else:
                        src = az.at[c, t - 1, g]
                        arrived(src, az_r.at[c, t - 1, g])
                        az[c, t - 1, g] = (acc + az[c, t - 1, g].astype(F32)).astype(BF16)
                    remote(src, az.at[c, t, g], send.at[0 if t == 0 else 1], az_r.at[c, t, g],
                           along(a_sign(c))).start()
                loop(groups, per_group)
            return body

        def a_turn(c, slot):
            def per_group(i):
                h, j = 1 - i // half, i % half
                g = group_at(c, 0, h, j)
                acc = product(slot, ra, g)
                arrived(az.at[c, ring - 2, g], az_r.at[c, ring - 2, g])
                az[c, ring - 2, g] = (acc + az[c, ring - 2, g].astype(F32)).astype(BF16)

                @pl.when(i < half)
                def _():
                    remote(az.at[c, ring - 2, g], ag.at[c, j], send.at[2], ag_r.at[c, 0], across(c, 0)).start()
            loop(groups, per_group)

        def a_stage(s):
            def body(c):
                n = half >> (s - 1)
                arrived(ag.at[c, pl.ds(off[s - 1], n)], ag_r.at[c, s - 1])

                def held(j):
                    if s == 1:
                        return az[c, ring - 2, group_at(c, 0, 0, j)]
                    return ag[c, off[s - 2] + slot_at(c, s - 1, 0, j)]

                def summed(j):
                    return ag[c, off[s - 1] + j].astype(F32) + held(j).astype(F32)

                if s == bits:
                    out[0, pl.ds(pl.multiple_of(c * ra, 16), ra), :] = summed(0)
                    return

                def per_slot(i):
                    h, jj = 1 - i // (n // 2), i % (n // 2)
                    j = slot_at(c, s, h, jj)
                    ag[c, off[s - 1] + j] = summed(j).astype(BF16)

                    @pl.when(i < n // 2)
                    def _():
                        remote(ag.at[c, off[s - 1] + j], ag.at[c, off[s] + jj], send.at[3],
                               ag_r.at[c, s], across(c, s)).start()
                loop(n, per_slot)
            return body

        def b_first(c, t, slot):
            o = c % 2

            def per_slot(j):
                acc = product(slot, rb, group_at(o, 0, 1, j))
                bsend[c, t, j] = acc.astype(BF16)
                remote(bsend.at[c, t, j], bg.at[c, t, j], send.at[4], bg_r.at[c, t, 0], across(o, 0)).start()
            loop(half, per_slot)

        def b_merge(c, t, s, add):
            o = c % 2
            n = half >> (s - 1)
            arrived(bg.at[c, t, pl.ds(off[s - 1], n)], bg_r.at[c, t, s - 1])

            def per_slot(i):
                h, jj = 1 - i // (n // 2), i % (n // 2)
                j = slot_at(o, s, h, jj)
                bg[c, t, off[s - 1] + j] = (add(j) + bg[c, t, off[s - 1] + j].astype(F32)).astype(BF16)

                @pl.when(i < n // 2)
                def _():
                    remote(bg.at[c, t, off[s - 1] + j], bg.at[c, t, off[s] + jj], send.at[5],
                           bg_r.at[c, t, s], across(o, s)).start()
            loop(n, per_slot)

        def b_second(c, t, slot):
            b_merge(c, t, 1, lambda j: product(slot, rb, group_at(c % 2, 0, 0, j)))

        def b_middle(p, s):
            def body(i):
                c, t = 2 * p + i % 2, i // 2
                b_merge(c, t, s, lambda j: bg[c, t, off[s - 2] + slot_at(c % 2, s - 1, 0, j)].astype(F32))
            loop(2 * ring, body)

        def b_ring(p, t):
            def body(i):
                c = 2 * p + i
                last = off[bits - 1]
                arrived(bg.at[c, t, pl.ds(last, 1)], bg_r.at[c, t, bits - 1])
                kept = off[bits - 2] + slot_at(c % 2, bits - 1, 0, 0)
                val = bg[c, t, last].astype(F32) + bg[c, t, kept].astype(F32)
                if t > 0:
                    arrived(bz.at[c, t - 1], bz_r.at[c, t - 1])
                    val = val + bz[c, t - 1].astype(F32)
                if t == ring - 1:
                    out[0, pl.ds(pl.multiple_of(2 * ra + c * rb, 16), rb), :] = val
                    return
                if t == 0:
                    src = bg.at[c, t, last]
                    bg[c, t, last] = val.astype(BF16)
                else:
                    src = bz.at[c, t - 1]
                    bz[c, t - 1] = val.astype(BF16)
                remote(src, bz.at[c, t], send.at[6], bz_r.at[c, t], along(b_sign(c))).start()
            loop(2, body)

        def a_site(t, body):
            return ("tiles", True, True, 2, lambda i: (i, t), lambda c, t_, slot: body(c, slot))

        def b_site(p, first, body):
            return ("tiles", False, first, 2 * ring, lambda i: (2 * p + i % 2, i // 2), body)

        def plain(fn):
            return ("plain", fn)

        def b_tail(p):
            middle = [plain(lambda s=s: b_middle(p, s)) for s in range(2, bits)]
            return middle + [plain(lambda t=t: b_ring(p, t)) for t in range(ring)]

        a_queue = [a_site(t, a_hop(t)) for t in range(1, ring - 1)] + [a_site(ring - 1, a_turn)]
        a_queue += [plain(lambda s=s: loop(2, a_stage(s))) for s in range(1, bits + 1)]
        queues, order = [], [b_site(0, True, b_first), a_site(0, a_hop(0))]

        def drain():
            for q in queues:
                if q:
                    order.append(q.pop(0))

        for p in range(PAIRS):
            order.append(b_site(p, False, b_second))
            if p + 1 == PAIRS:
                break
            order.append(b_site(p + 1, True, b_first))
            queues.append(b_tail(p))
            drain()
            if len(a_queue) > bits + 1:
                order.append(a_queue.pop(0))
            drain()
        queues.append(b_tail(PAIRS - 1))
        while a_queue or any(queues):
            if a_queue:
                order.append(a_queue.pop(0))
            drain()

        def begin(site, i, slot):
            _, is_a, first, _, index, _ = site
            c, t = index(i)
            sgn = a_sign(c) if is_a else b_sign(c)
            own, other = tile_copies(is_a, c, t, sgn, slot)
            own.start()
            if is_a:
                arrived(wxa.at[c, t], wa_r.at[c, t])
            elif first:
                @pl.when(t == 0)
                def _():
                    arrived(wxb.at[c], wb_r.at[c])
            other.start()

        tiles = [s for s in order if s[0] == "tiles"]
        begin(tiles[0], 0, 0)
        at = 0
        for site in order:
            if site[0] == "plain":
                site[1]()
                continue
            at += 1
            follow = tiles[at] if at < len(tiles) else None
            _, is_a, first, count, index, body = site

            def run(i, site=site, follow=follow, is_a=is_a, count=count, index=index, body=body):
                slot = i % 2

                @pl.when(i + 1 < count)
                def _():
                    begin(site, i + 1, 1 - slot)

                if follow is not None:
                    @pl.when(i + 1 == count)
                    def _():
                        begin(follow, 0, 1 - slot)
                c, t = index(i)
                for cp in tile_copies(is_a, c, t, a_sign(c) if is_a else b_sign(c), slot):
                    cp.wait()
                body(c, t, slot)
            loop(count, run)

        x_copy.wait_send()
        arrived(wxa, w_s.at[0])
        arrived(wxb, w_s.at[1])
        arrived(asend, send.at[0])
        arrived(az.at[:, pl.ds(0, ring - 2)], send.at[1])
        arrived(ag.at[:, pl.ds(0, half)], send.at[2])
        arrived(ag.at[:, pl.ds(0, half - 1)], send.at[3])
        arrived(bsend, send.at[4])
        arrived(bg.at[:, :, pl.ds(0, half - 1)], send.at[5])
        arrived(bz, send.at[6])

    dma = pltpu.SemaphoreType.DMA
    nb = 2 * PAIRS
    shapes = [
        pltpu.VMEM((splits, depth, cols), BF16),
        pltpu.VMEM((groups, 2 * depth, cols), BF16),
        pltpu.VMEM((2, 2, blocks, max(ra, rb), depth), BF16),
        pltpu.VMEM((max(ra, rb), 2 * depth), BF16),
        pltpu.VMEM((2, groups, ra, cols), BF16),
        pltpu.VMEM((2, ring - 1, groups, ra, cols), BF16),
        pltpu.VMEM((2, groups - 1, ra, cols), BF16),
        pltpu.VMEM((nb, ring, half, rb, cols), BF16),
        pltpu.VMEM((nb, ring, groups - 1, rb, cols), BF16),
        pltpu.VMEM((nb, ring - 1, rb, cols), BF16),
        dma, dma, dma((2,)), dma((2, ring)), dma((nb,)), dma((2, 2)), dma((7,)),
        dma((2, ring - 1, groups)), dma((2, bits)), dma((nb, ring, bits)), dma((nb, ring - 1)),
    ]
    spaces = (pltpu.VMEM, pl.ANY, pl.ANY)
    return pl.pallas_call(
        kernel,
        name="coded_share",
        out_shape=(
            jax.ShapeDtypeStruct((1, rows, cols), F32),
            jax.ShapeDtypeStruct((2, ring, blocks, ra, depth), BF16),
            jax.ShapeDtypeStruct((nb, ring, blocks, rb, depth), BF16),
        ),
        in_specs=[
            pl.BlockSpec(memory_space=pltpu.SMEM),
            pl.BlockSpec(memory_space=pl.ANY),
            pl.BlockSpec(memory_space=pltpu.VMEM),
        ],
        out_specs=tuple(pl.BlockSpec(memory_space=m) for m in spaces),
        scratch_shapes=shapes,
        compiler_params=pltpu.CompilerParams(
            collective_id=0, has_side_effects=True, vmem_limit_bytes=67043328),
    )


def solution(mesh):
    groups, members = mesh.shape["grp"], mesh.shape["mem"]

    def per_device(weight, activation, points):
        blocks, height, depth = weight.shape
        splits, _, cols = activation.shape
        rows = height // members
        rb = (rows * 13 // 16) // (2 * PAIRS) // 16 * 16
        ra = (rows - 2 * PAIRS * rb) // 2
        call = make_kernel(groups, members, blocks, splits, rows, depth, cols, ra, rb)
        return call(points, weight, activation)[0]

    placed = (P(None, None, ("grp", "mem")), P(None, ("grp", "mem"), None), P())
    return jax.shard_map(
        per_device, mesh=mesh, in_specs=placed, out_specs=P("grp", "mem", None), check_vma=False)
```
